32 devices in a mesh: rows: 4 (over x, core), cols: 8 (over z, y).
Axes of the slice: x: 2, y: 2, z: 4, core: 2. Of those that a mesh axis runs over, the one named last changes fastest.
Arguments:
- elevation: float32 [512, 8192], P('rows', 'cols'), may hold values from -6 to 6
- data_mask: int32 [512, 8192], P('rows', 'cols'), may hold values 0 or 1
- tie_order: int32 [8], replicated, may hold values from 0 to 7, each once
Outputs:
- inflow: float32 [512, 8192], P('rows', 'cols')
The draws below stay inside these ranges and needn't reach their ends.
Inputs may be any that keep to these rules, and one draw needn't show every extreme that they name: tie_order holds each of 0 to 7 once.
All inputs are finite; a program needn't handle non-finite values. No bound on the sum of `data_mask` on one device may be relied on, other than what follows from the above.
Results may differ from the reference program's by a relative error of at most 0.0003.
Values sent between devices are 32-bit elements; how exact they have to be, the bound alone decides.
A program may use at most 64 MiB of HBM per device.

```python
import jax
import jax.numpy as jnp
from jax import lax

TILE_COLUMNS = 1024
ITERS = 8
NR = 512
NC = 8192
N_COLS = 8


def plant(drawn, stream_key, low, high):
    spot = [jax.random.randint(jax.random.fold_in(stream_key, axis), (), 0, length) for axis, length in enumerate(drawn.shape)]
    widest = drawn.shape.index(max(drawn.shape))
    next_to = spot[:widest] + [(spot[widest] + 1) % drawn.shape[widest]] + spot[widest + 1:]
    return drawn.at[tuple(spot)].set(low).at[tuple(next_to)].set(high)


def block_levels(key, dims, shards, smallest, high):
    def one(axis_at, shards_of):
        heights = jax.random.uniform(jax.random.fold_in(jax.random.fold_in(key, 6), axis_at), (shards_of,), jnp.float32, smallest / len(shards), high / len(shards))
        return jnp.repeat(jnp.exp(heights), dims[axis_at] // shards_of).reshape((-1,) + (1,) * (len(dims) - axis_at - 1))

    level = one(*shards[0])
    for cut in shards[1:]:
        level = level * one(*cut)
    return level


def gaussian(key, shape, width, limit, shards=(), kind=jnp.bfloat16):
    drawn = jax.random.normal(key, shape, jnp.float32) * width
    if len(shards) > 0:
        drawn = block_levels(key, shape, shards, -0.22, 0.18) * drawn
    return jnp.clip(drawn, min=-limit, max=limit).astype(kind)


def setup_inputs(seed: int = 0) -> dict:
    key_list = jax.random.split(jax.random.key(seed), 4)
    return {
        "elevation": gaussian(key_list[0], (NR, NC), 1.0, 6.0, ((0, 4), (1, 8)), jnp.float32),
        "data_mask": plant((jax.random.randint(key_list[1], (NR, NC), 0, 4) < 3).astype(jnp.int32), jax.random.fold_in(key_list[1], 1), 0, 1),
        "tie_order": jax.random.permutation(key_list[2], 8).astype(jnp.int32),
    }


OFFSETS = ((0, 1), (1, 1), (1, 0), (1, -1), (0, -1), (-1, -1), (-1, 0), (-1, 1))
RECIPROCAL = (1.0, 0.7071067811865476, 1.0, 0.7071067811865476, 1.0, 0.7071067811865476, 1.0, 0.7071067811865476)
RETENTION = 0.1


def priorities(tie_order):
    places = jnp.arange(8, dtype=jnp.float32)
    values = 1.0 + 0.5 * (7.0 - places) / 7.0
    matches = (tie_order[:, None] == jnp.arange(8, dtype=jnp.int32)[None, :]).astype(jnp.float32)
    return jnp.sum(matches * values[:, None], axis=0)


def outflow_weight_matrix(height_pad, valid_pad, ranking_order):
    height = height_pad.shape[0] - 2
    breadth = height_pad.shape[1] - 2
    centre = height_pad[1:-1, 1:-1]
    slopes = []
    for number, (step_row, step_col) in enumerate(OFFSETS):
        beside = height_pad[1 + step_row:1 + step_row + height, 1 + step_col:1 + step_col + breadth]
        beside_ok = valid_pad[1 + step_row:1 + step_row + height, 1 + step_col:1 + step_col + breadth]
        slopes.append(beside_ok * ranking_order[number] * jnp.maximum(centre - beside, 0.0) * RECIPROCAL[number])
    slopes = jnp.stack(slopes)
    totals = jnp.sum(slopes, axis=0) + RETENTION
    return slopes / totals


def gather_inflow(weights, field_pad):
    height = field_pad.shape[0] - 2
    breadth = field_pad.shape[1] - 2
    summed_in = jnp.zeros((height, breadth), jnp.float32)
    for number, (step_row, step_col) in enumerate(OFFSETS):
        term = weights[number] * field_pad
        summed_in = summed_in + term[1 - step_row:1 - step_row + height, 1 - step_col:1 - step_col + breadth]
    return summed_in


def reference(elevation, data_mask, tie_order):
    ranking_order = priorities(tie_order)
    full_rows, full_cols = elevation.shape
    valid_flag = data_mask.astype(jnp.float32)
    over_rows, over_cols = full_rows // 8, full_cols // 8
    summed = (valid_flag * elevation).reshape(over_rows, 8, over_cols, 8).sum(axis=(1, 3))
    counts = valid_flag.reshape(over_rows, 8, over_cols, 8).sum(axis=(1, 3))
    overview = summed / (counts + 1.0)
    runoff = counts / 64.0
    coarse_w = outflow_weight_matrix(jnp.pad(overview, 2), jnp.pad(jnp.ones_like(overview), 2), ranking_order)
    flow_now = runoff
    for sweep in range(ITERS):
        flow_now = runoff + gather_inflow(coarse_w, jnp.pad(flow_now, 1))
    upsampled = jnp.repeat(jnp.repeat(flow_now, 8, axis=0), 8, axis=1)
    up_window = jnp.pad(upsampled, 1)
    elevation_window = jnp.pad(elevation, 2)
    valid_cols = jnp.pad(jnp.ones((full_cols,), jnp.float32), 2)
    valid_rows = jnp.pad(jnp.ones((full_rows,), jnp.float32), 2)

    def one_block(column_block):
        start_offset = (column_block * TILE_COLUMNS).astype(jnp.int32)
        height_values = lax.dynamic_slice_in_dim(elevation_window, start_offset, TILE_COLUMNS + 4, 1)
        valid_pad = valid_rows[:, None] * lax.dynamic_slice_in_dim(valid_cols, start_offset, TILE_COLUMNS + 4, 0)[None, :]
        ups = lax.dynamic_slice_in_dim(up_window, start_offset, TILE_COLUMNS + 2, 1)
        flags = lax.dynamic_slice_in_dim(valid_flag, start_offset, TILE_COLUMNS, 1)
        detailed_weight = outflow_weight_matrix(height_values, valid_pad, ranking_order)
        return flags + gather_inflow(detailed_weight, ups)

    blocks = lax.map(one_block, jnp.arange(N_COLS, dtype=jnp.int32))
    return jnp.moveaxis(blocks, 0, 1).reshape(full_rows, full_cols)
```

```python
import functools

import jax
import jax.numpy as jnp
from jax import lax
from jax.experimental import pallas as pl
from jax.experimental.pallas import tpu as pltpu
from jax.sharding import PartitionSpec as P

ITERS = 8
OFFSETS = ((0, 1), (1, 1), (1, 0), (1, -1), (0, -1), (-1, -1), (-1, 0), (-1, 1))
RECIPROCAL = (1.0, 0.7071067811865476) * 4
RETENTION = 0.1
OUTSIDE = 1000.0
LANES = 128
F32 = jnp.float32


def coefficients(tie_ref):
    out = []
    for k in range(8):
        value = jnp.float32(0.0)
        for i in range(8):
            place = jnp.float32((1.0 + 0.5 * (7.0 - i) / 7.0) * RECIPROCAL[k])
            value = jnp.where(tie_ref[i] == k, place, value)
        out.append(value)
    return out


def shift_lanes(before, here, after, step, lane):
    if step == 0:
        return here
    if step < 0:
        return pltpu.roll(jnp.where(lane == LANES - 1, before, here), 1, 1)
    return pltpu.roll(jnp.where(lane == 0, after, here), LANES - 1, 1)


def take_lanes(values, index):
    return jnp.take_along_axis(values, index, axis=1, mode="promise_in_bounds")


def kernel(row_devices, col_devices, tie_ref, elev_ref, mask_ref, out_ref, zp, mask, recip, parts, ones,
           coarse, crecv, load_sem, send_sem, recv_sem):
    rows, cols = elev_ref.shape
    groups, blocks = rows // 8, cols // LANES
    row, col = lax.axis_index("rows"), lax.axis_index("cols")

    loads = []
    for j in range(blocks):
        part = pl.ds(j * LANES, LANES)
        loads.append(pltpu.make_async_copy(elev_ref.at[:, part], zp.at[j + 1, pl.ds(8, rows), :], load_sem.at[j]))
        loads.append(pltpu.make_async_copy(mask_ref.at[:, part], mask.at[j], load_sem.at[blocks + j]))
    for load in loads:
        load.start()

    barrier = pltpu.get_barrier_semaphore()
    exists = []
    for step_row, step_col in OFFSETS:
        there = jnp.bool_(True)
        if step_row > 0:
            there = row < row_devices - 1
        if step_row < 0:
            there = row > 0
        if step_col > 0:
            there = jnp.logical_and(there, col < col_devices - 1)
        if step_col < 0:
            there = jnp.logical_and(there, col > 0)
        exists.append(there)

    def peer(k):
        return {"rows": row + OFFSETS[k][0], "cols": col + OFFSETS[k][1]}

    for k in range(8):
        @pl.when(exists[k])
        def _():
            pl.semaphore_signal(barrier, inc=1, device_id=peer(k), device_id_type=pl.DeviceIdType.MESH)

    coef = coefficients(tie_ref)

    def halo(step_row, step_col):
        where_rows = {-1: pl.ds(0, 8), 0: pl.ds(8, rows), 1: pl.ds(8 + rows, 8)}[step_row]
        where_blocks = {-1: pl.ds(0, 1), 0: pl.ds(1, blocks), 1: pl.ds(blocks + 1, 1)}[step_col]
        return zp.at[where_blocks, where_rows, :]

    def edge(step_row, step_col):
        where_rows = {-1: pl.ds(8, 8), 0: pl.ds(8, rows), 1: pl.ds(rows, 8)}[step_row]
        where_blocks = {-1: pl.ds(1, 1), 0: pl.ds(1, blocks), 1: pl.ds(blocks, 1)}[step_col]
        return zp.at[where_blocks, where_rows, :]

    crows = groups
    for k in range(8):
        @pl.when(jnp.logical_not(exists[k]))
        def _():
            region = halo(*OFFSETS[k])
            region[...] = jnp.full(region.shape, OUTSIDE, F32)
            crecv[k, 0:crows, :] = jnp.full((crows, LANES), OUTSIDE, F32)
            crecv[k, crows:2 * crows, :] = jnp.zeros((crows, LANES), F32)

    ones[...] = (
        lax.broadcasted_iota(jnp.int32, (cols, LANES), 0) // 8 == lax.broadcasted_iota(jnp.int32, (cols, LANES), 1)
    ).astype(F32).astype(jnp.bfloat16)

    for load in loads:
        load.wait()

    total = jnp.zeros((4 * crows, LANES), F32)
    for j in range(blocks):
        height_sum = jnp.zeros((crows, LANES), F32)
        count_sum = jnp.zeros((crows, LANES), F32)
        for s in range(8):
            valid = mask[j, pl.ds(s, crows, stride=8), :].astype(F32)
            height_sum = height_sum + valid * zp[j + 1, pl.ds(8 + s, crows, stride=8), :]
            count_sum = count_sum + valid
        high = height_sum.astype(jnp.bfloat16)
        rest = height_sum - high.astype(F32)
        middle = rest.astype(jnp.bfloat16)
        low = (rest - middle.astype(F32)).astype(jnp.bfloat16)
        stacked = jnp.concatenate([count_sum.astype(jnp.bfloat16), high, middle, low], axis=0)
        total = total + jnp.dot(stacked, ones[j * LANES:(j + 1) * LANES, :], preferred_element_type=F32)
    counts = total[0:crows]
    heights = total[crows:2 * crows] + (total[2 * crows:3 * crows] + total[3 * crows:])
    overview = heights / (counts + 1.0)
    runoff = counts * (1.0 / 64.0)
    coarse[0:crows, :] = overview
    coarse[crows:2 * crows, :] = runoff

    pl.semaphore_wait(barrier, functools.reduce(jnp.add, [there.astype(jnp.int32) for there in exists]))

    def copies(k):
        opposite = (k + 4) % 8
        small = pltpu.make_async_remote_copy(
            src_ref=coarse, dst_ref=crecv.at[opposite], send_sem=send_sem.at[k], recv_sem=recv_sem.at[opposite],
            device_id=peer(k), device_id_type=pl.DeviceIdType.MESH)
        step_row, step_col = OFFSETS[k]
        large = pltpu.make_async_remote_copy(
            src_ref=edge(step_row, step_col), dst_ref=halo(-step_row, -step_col),
            send_sem=send_sem.at[8 + k], recv_sem=recv_sem.at[8 + opposite],
            device_id=peer(k), device_id_type=pl.DeviceIdType.MESH)
        return small, large

    def arrivals(k):
        small = pltpu.make_async_remote_copy(
            src_ref=coarse, dst_ref=crecv.at[k], send_sem=send_sem.at[k], recv_sem=recv_sem.at[k],
            device_id=peer(k), device_id_type=pl.DeviceIdType.MESH)
        step_row, step_col = OFFSETS[k]
        large = pltpu.make_async_remote_copy(
            src_ref=edge(step_row, step_col), dst_ref=halo(step_row, step_col),
            send_sem=send_sem.at[8 + k], recv_sem=recv_sem.at[8 + k],
            device_id=peer(k), device_id_type=pl.DeviceIdType.MESH)
        return small, large

    for which in range(2):
        for k in (1, 3, 5, 7, 0, 4, 2, 6):
            @pl.when(exists[k])
            def _():
                copies(k)[which].start()

    for k in range(8):
        @pl.when(exists[k])
        def _():
            arrivals(k)[1].wait_recv()

    lane = lax.broadcasted_iota(jnp.int32, (8, LANES), 1)
    sub = lax.broadcasted_iota(jnp.int32, (8, LANES), 0)

    def first_pass(g, carry):
        for j in range(blocks + 2):
            here = zp[j, pl.ds(8 * g + 7, 8), :]
            summed = jnp.full((8, LANES), RETENTION, F32)
            for step_row in (-1, 0, 1):
                at = pl.ds(8 * g + 7 + step_row, 8)
                line = [zp[min(max(b, 0), blocks + 1), at, :] for b in (j - 1, j, j + 1)]
                for k, (off_row, off_col) in enumerate(OFFSETS):
                    if off_row == step_row:
                        beside = shift_lanes(*line, off_col, lane)
                        summed = summed + coef[k] * jnp.maximum(here - beside, 0.0)
            recip[j, pl.ds(8 * g + 7, 8), :] = 1.0 / summed
        return carry

    lax.fori_loop(0, groups + 1, first_pass, 0)

    def second_pass(g, carry):
        for j in range(1, blocks + 1):
            here = zp[j, pl.ds(pl.multiple_of(8 * g + 8, 8), 8), :]
            inside, rim = {}, {}
            for step_col in (-1, 0, 1):
                terms = {}
                for step_row in (-1, 0, 1):
                    if (step_row, step_col) == (0, 0):
                        continue
                    k = OFFSETS.index((-step_row, -step_col))
                    at = pl.ds(8 * g + 8 + step_row, 8)
                    source = shift_lanes(zp[j - 1, at, :], zp[j, at, :], zp[j + 1, at, :], step_col, lane)
                    scale = shift_lanes(recip[j - 1, at, :], recip[j, at, :], recip[j + 1, at, :], step_col, lane)
                    terms[step_row] = coef[k] * jnp.maximum(source - here, 0.0) * scale
                inside[step_col] = jnp.where(sub == 0, 0.0, terms[-1]) + jnp.where(sub == 7, 0.0, terms[1])
                if step_col != 0:
                    inside[step_col] = inside[step_col] + terms[0]
                rim[step_col] = jnp.where(sub == 0, terms[-1], jnp.where(sub == 7, terms[1], 0.0))
            first, last = (lane & 7) == 0, (lane & 7) == 7
            at = pl.ds(pl.multiple_of(8 * g, 8), 8)
            for number, field in enumerate((inside, rim)):
                parts[2 * number, j - 1, at, :] = (
                    field[0] + jnp.where(first, 0.0, field[-1]) + jnp.where(last, 0.0, field[1])
                )
                parts[2 * number + 1, j - 1, at, :] = jnp.where(first, field[-1], jnp.where(last, field[1], 0.0))
        return carry

    lax.fori_loop(0, groups, second_pass, 0)

    for k in range(8):
        @pl.when(exists[k])
        def _():
            arrivals(k)[0].wait_recv()

    lane_c = lax.broadcasted_iota(jnp.int32, (crows, LANES), 1)
    half = crows // 2

    def window(base):
        def side(right, left):
            return jnp.where(
                lane_c < LANES // 2, crecv[right, base:base + crows, :], crecv[left, base:base + crows, :])

        own = jnp.concatenate([coarse[base:base + crows, :], side(0, 4)], axis=1)
        below = jnp.concatenate([crecv[2, base:base + crows, :], side(1, 3)], axis=1)
        above = jnp.concatenate([crecv[6, base:base + crows, :], side(7, 5)], axis=1)
        sub_w = lax.broadcasted_iota(jnp.int32, (8, 2 * LANES), 0)
        mixed = jnp.where(sub_w < 4, below[8:16], above[crows - 16:crows - 8])
        return jnp.concatenate([own, below[0:8], mixed, above[crows - 8:crows]], axis=0)

    z = window(0)
    supply = window(crows)
    high, wide = z.shape

    def turn(x, step, axis):
        return x if step == 0 else pltpu.roll(x, (-step) % x.shape[axis], axis)

    turned = {step: turn(z, step, 1) for step in (-1, 0, 1)}
    slopes = []
    for k, (step_row, step_col) in enumerate(OFFSETS):
        slopes.append(coef[k] * jnp.maximum(z - turn(turned[step_col], step_row, 0), 0.0))
    share = 1.0 / (functools.reduce(jnp.add, slopes) + RETENTION)
    weight = {}
    for k, (step_row, step_col) in enumerate(OFFSETS):
        weight[step_row, step_col] = turn(slopes[k] * share, -step_col, 1)
    flow = supply
    for _ in range(ITERS):
        moved = {step: turn(flow, -step, 1) for step in (-1, 0, 1)}
        sums = {}
        for step_row in (-1, 0, 1):
            sums[step_row] = functools.reduce(
                jnp.add, [weight[step_row, c] * moved[c] for c in (-1, 0, 1) if (step_row, c) in weight])
        flow = supply + sums[0] + turn(sums[1], -1, 0) + turn(sums[-1], 1, 0)

    left = turn(flow, -1, 1)[:, :LANES]
    right = turn(flow, 1, 1)[:, :LANES]
    centre = flow[:, :LANES]
    first, last = (lane & 7) == 0, (lane & 7) == 7
    per_block = LANES // 8
    for j in range(blocks):
        index = lane // 8 + j * per_block
        spread = []
        for at in list(range(0, crows, 8)) + [crows, high - 8]:
            mid = take_lanes(centre[at:at + 8], index)
            beside = jnp.where(first, take_lanes(left[at:at + 8], index), take_lanes(right[at:at + 8], index))
            spread.append((mid, beside))
        for g in range(groups):
            def level(number, group):
                where_at = {-1: (len(spread) - 1, 7), groups: (len(spread) - 2, 0)}.get(group, (group // 8, group % 8))
                line = spread[where_at[0]][number][where_at[1]:where_at[1] + 1, :]
                return jnp.broadcast_to(line, (8, LANES))

            at = slice(8 * g, 8 * g + 8)
            value = mask[j, at, :].astype(F32)
            for number in range(2):
                value = value + parts[number, j, at, :] * level(number, g)
                rim = jnp.where(sub == 0, level(number, g - 1), level(number, g + 1))
                value = value + parts[2 + number, j, at, :] * rim
            out_ref[at, j * LANES:(j + 1) * LANES] = value

    for k in range(8):
        @pl.when(exists[k])
        def _():
            small, large = copies(k)
            small.wait_send()
            large.wait_send()


def solution(mesh):
    row_devices, col_devices = mesh.shape["rows"], mesh.shape["cols"]

    def on_device(elevation, data_mask, tie_order):
        rows, cols = elevation.shape
        groups, blocks = rows // 8, cols // LANES
        return pl.pallas_call(
            functools.partial(kernel, row_devices, col_devices),
            out_shape=jax.ShapeDtypeStruct((rows, cols), F32),
            in_specs=[
                pl.BlockSpec(memory_space=pltpu.SMEM),
                pl.BlockSpec(memory_space=pl.ANY),
                pl.BlockSpec(memory_space=pl.ANY),
            ],
            out_specs=pl.BlockSpec(memory_space=pltpu.VMEM),
            scratch_shapes=[
                pltpu.VMEM((blocks + 2, rows + 16, LANES), F32),
                pltpu.VMEM((blocks, rows, LANES), jnp.int32),
                pltpu.VMEM((blocks + 2, rows + 16, LANES), F32),
                pltpu.VMEM((4, blocks, rows, LANES), F32),
                pltpu.VMEM((cols, LANES), jnp.bfloat16),
                pltpu.VMEM((2 * groups, LANES), F32),
                pltpu.VMEM((8, 2 * groups, LANES), F32),
                pltpu.SemaphoreType.DMA((2 * blocks,)),
                pltpu.SemaphoreType.DMA((16,)),
                pltpu.SemaphoreType.DMA((16,)),
            ],
            compiler_params=pltpu.CompilerParams(collective_id=0, has_side_effects=True),
        )(tie_order, elevation, data_mask)

    return jax.shard_map(
        on_device, mesh=mesh, in_specs=(P("rows", "cols"), P("rows", "cols"), P()),
        out_specs=P("rows", "cols"), check_vma=False)
```

```python
import functools

import jax
import jax.numpy as jnp
from jax import lax
from jax.experimental import pallas as pl
from jax.experimental.pallas import tpu as pltpu
from jax.sharding import PartitionSpec as P

ITERS = 8
OFFSETS = ((0, 1), (1, 1), (1, 0), (1, -1), (0, -1), (-1, -1), (-1, 0), (-1, 1))
RECIPROCAL = (1.0, 0.7071067811865476) * 4
RETENTION = 0.1
OUTSIDE = 1000.0
LANES = 128
F32 = jnp.float32


def coefficients(tie_ref):
    out = []
    for k in range(8):
        value = jnp.float32(0.0)
        for i in range(8):
            place = jnp.float32((1.0 + 0.5 * (7.0 - i) / 7.0) * RECIPROCAL[k])
            value = jnp.where(tie_ref[i] == k, place, value)
        out.append(value)
    return out


def shift_lanes(before, here, after, step, lane):
    if step == 0:
        return here
    if step < 0:
        return pltpu.roll(jnp.where(lane == LANES - 1, before, here), 1, 1)
    return pltpu.roll(jnp.where(lane == 0, after, here), LANES - 1, 1)


def take_lanes(values, index):
    return jnp.take_along_axis(values, index, axis=1, mode="promise_in_bounds")


def kernel(row_devices, col_devices, tie_hbm, elev_ref, mask_ref, out_ref, tie_ref, zp, mask, recip, parts, ones,
           coarse, side, srecv, vrecv, load_sem, tie_sem, send_sem, recv_sem):
    rows, cols = elev_ref.shape
    groups, blocks = rows // 8, cols // LANES
    crows = groups
    row, col = lax.axis_index("rows"), lax.axis_index("cols")
    ring, rim = 0, blocks + 1

    loads = []
    for j in range(blocks):
        part = pl.ds(j * LANES, LANES)
        loads.append((
            pltpu.make_async_copy(elev_ref.at[:, part], zp.at[j + 1, pl.ds(8, rows), :], load_sem.at[j]),
            pltpu.make_async_copy(mask_ref.at[:, part], mask.at[j], load_sem.at[blocks + j])))
        loads[-1][0].start()
        loads[-1][1].start()
    tie_load = pltpu.make_async_copy(tie_hbm, tie_ref, tie_sem)
    tie_load.start()

    barrier = pltpu.get_barrier_semaphore()
    exists = []
    for step_row, step_col in OFFSETS:
        there = jnp.bool_(True)
        if step_row > 0:
            there = row < row_devices - 1
        if step_row < 0:
            there = row > 0
        if step_col > 0:
            there = jnp.logical_and(there, col < col_devices - 1)
        if step_col < 0:
            there = jnp.logical_and(there, col > 0)
        exists.append(there)

    def peer(k):
        return {"rows": row + OFFSETS[k][0], "cols": col + OFFSETS[k][1]}

    for k in range(8):
        @pl.when(exists[k])
        def _():
            pl.semaphore_signal(barrier, inc=1, device_id=peer(k), device_id_type=pl.DeviceIdType.MESH)

    lane = lax.broadcasted_iota(jnp.int32, (8, LANES), 1)
    sub = lax.broadcasted_iota(jnp.int32, (8, LANES), 0)
    lane_c = lax.broadcasted_iota(jnp.int32, (crows, LANES), 1)
    middle_lanes = jnp.logical_and(lane_c >= LANES // 4, lane_c < 3 * LANES // 4)

    SIDES, UPDOWN = (0, 1, 3, 4, 5, 7), (2, 6)

    def halo_rows(k):
        return zp.at[pl.ds(1, blocks), pl.ds(8 + rows if k == 2 else 0, 8), :]

    def edge_rows(k):
        return zp.at[pl.ds(1, blocks), pl.ds(rows if k == 2 else 8, 8), :]

    for k in range(8):
        @pl.when(jnp.logical_not(exists[k]))
        def _():
            if k in UPDOWN:
                region = halo_rows(k)
                region[...] = jnp.full(region.shape, OUTSIDE, F32)
                vrecv[k // 4, 0:crows, :] = jnp.full((crows, LANES), OUTSIDE, F32)
                vrecv[k // 4, crows:2 * crows, :] = jnp.zeros((crows, LANES), F32)
            else:
                srecv[k, 0:crows, :] = jnp.where(middle_lanes, 0.0, OUTSIDE)
                srecv[k, crows:crows + 8, :] = jnp.full((8, LANES), OUTSIDE, F32)

    ones[...] = (
        lax.broadcasted_iota(jnp.int32, (cols, LANES), 0) // 8 == lax.broadcasted_iota(jnp.int32, (cols, LANES), 1)
    ).astype(F32).astype(jnp.bfloat16)

    total = jnp.zeros((4 * crows, LANES), F32)
    for j in range(blocks):
        loads[j][0].wait()
        loads[j][1].wait()
        height_sum = jnp.zeros((crows, LANES), F32)
        count_sum = jnp.zeros((crows, LANES), F32)
        for s in range(8):
            valid = mask[j, pl.ds(s, crows, stride=8), :].astype(F32)
            height_sum = height_sum + valid * zp[j + 1, pl.ds(8 + s, crows, stride=8), :]
            count_sum = count_sum + valid
        high = height_sum.astype(jnp.bfloat16)
        rest = height_sum - high.astype(F32)
        middle = rest.astype(jnp.bfloat16)
        low = (rest - middle.astype(F32)).astype(jnp.bfloat16)
        stacked = jnp.concatenate([count_sum.astype(jnp.bfloat16), high, middle, low], axis=0)
        total = total + jnp.dot(stacked, ones[j * LANES:(j + 1) * LANES, :], preferred_element_type=F32)
    counts = total[0:crows]
    heights = total[crows:2 * crows] + (total[2 * crows:3 * crows] + total[3 * crows:])
    overview = heights / (counts + 1.0)
    runoff = counts * (1.0 / 64.0)

    packed = jnp.zeros((8, LANES), F32)
    for g in range(groups):
        at = pl.ds(8 + 8 * g, 8)
        edges = jnp.where(lane < LANES // 2, zp[1, at, :], zp[blocks, at, :])
        zp[rim, at, :] = edges
        packed = jnp.where(lane // 4 == g, pltpu.roll(edges, (2 + 4 * g) % LANES, 1), packed)
    side[crows:crows + 8, :] = packed
    side[0:crows, :] = jnp.where(middle_lanes, pltpu.roll(runoff, LANES // 2, 1), overview)
    coarse[0:crows, :] = overview
    coarse[crows:2 * crows, :] = runoff

    pl.semaphore_wait(barrier, functools.reduce(jnp.add, [there.astype(jnp.int32) for there in exists]))

    def copies(k, arriving=False):
        slot = k if arriving else (k + 4) % 8

        def remote(src, dst, extra):
            return pltpu.make_async_remote_copy(
                src_ref=src, dst_ref=dst, send_sem=send_sem.at[k + extra], recv_sem=recv_sem.at[slot + extra],
                device_id=peer(k), device_id_type=pl.DeviceIdType.MESH)

        if k in UPDOWN:
            return [remote(coarse, vrecv.at[slot // 4], 0), remote(edge_rows(k), halo_rows(slot), 8)]
        return [remote(side, srecv.at[slot], 0)]

    for k in (1, 3, 5, 7, 0, 4, 2, 6):
        @pl.when(exists[k])
        def _():
            for copy in copies(k):
                copy.start()

    tie_load.wait()
    coef = coefficients(tie_ref)

    def first_pass(g, around):
        for j, before, after in around:
            here = zp[j, pl.ds(8 * g + 7, 8), :]
            summed = jnp.full((8, LANES), RETENTION, F32)
            for step_row in (-1, 0, 1):
                at = pl.ds(8 * g + 7 + step_row, 8)
                line = [zp[b, at, :] for b in (before, j, after)]
                for k, (off_row, off_col) in enumerate(OFFSETS):
                    if off_row == step_row:
                        beside = shift_lanes(*line, off_col, lane)
                        summed = summed + coef[k] * jnp.maximum(here - beside, 0.0)
            recip[j, pl.ds(8 * g + 7, 8), :] = 1.0 / summed

    def second_pass(g, around, store):
        for j, before, after in around:
            here = zp[j, pl.ds(8 * g + 8, 8), :]
            inside, outer = {}, {}
            for step_col in (-1, 0, 1):
                terms = {}
                for step_row in (-1, 0, 1):
                    if (step_row, step_col) == (0, 0):
                        continue
                    k = OFFSETS.index((-step_row, -step_col))
                    at = pl.ds(8 * g + 8 + step_row, 8)
                    source = shift_lanes(zp[before, at, :], zp[j, at, :], zp[after, at, :], step_col, lane)
                    scale = shift_lanes(recip[before, at, :], recip[j, at, :], recip[after, at, :], step_col, lane)
                    terms[step_row] = coef[k] * jnp.maximum(source - here, 0.0) * scale
                inside[step_col] = jnp.where(sub == 0, 0.0, terms[-1]) + jnp.where(sub == 7, 0.0, terms[1])
                if step_col != 0:
                    inside[step_col] = inside[step_col] + terms[0]
                outer[step_col] = jnp.where(sub == 0, terms[-1], jnp.where(sub == 7, terms[1], 0.0))
            first, last = (lane & 7) == 0, (lane & 7) == 7
            for number, field in enumerate((inside, outer)):
                store(g, j, 2 * number, field[0] + jnp.where(first, 0.0, field[-1]) + jnp.where(last, 0.0, field[1]))
                store(g, j, 2 * number + 1, jnp.where(first, field[-1], jnp.where(last, field[1], 0.0)))

    def keep(g, j, number, value):
        parts[number, j - 1, pl.ds(8 * g, 8), :] = value

    def keep_edges(g, j, number, value):
        at = pl.ds(8 * g, 8)
        parts[number, 0, at, :] = jnp.where(lane < 8, value, parts[number, 0, at, :])
        parts[number, blocks - 1, at, :] = jnp.where(lane >= LANES - 8, value, parts[number, blocks - 1, at, :])

    own = [(j, j - 1, j + 1 if j < blocks else ring) for j in range(1, blocks + 1)]
    outside, edges = (ring, blocks, 1), (rim, ring, ring)

    def loop(start, stop, body):
        def step(g, carry):
            body(g)
            return carry

        lax.fori_loop(start, stop, step, 0)

    loop(1, groups, lambda g: first_pass(g, own))
    loop(1, groups - 1, lambda g: second_pass(g, own, keep))

    for k in range(8):
        @pl.when(exists[k])
        def _():
            for copy in copies(k, arriving=True):
                copy.wait_recv()

    def outside_columns(g, right, left):
        chosen = jnp.where(lane >= 4 * g + 2, srecv[right, crows:crows + 8, :], srecv[left, crows:crows + 8, :])
        return pltpu.roll(chosen, (2 * LANES - 4 * g - 2) % LANES, 1)

    for g in range(groups):
        zp[ring, pl.ds(8 + 8 * g, 8), :] = outside_columns(g, 0, 4)
    zp[ring, 0:8, :] = outside_columns(groups - 1, 7, 5)
    zp[ring, rows + 8:rows + 16, :] = outside_columns(0, 1, 3)
    for at in (0, rows + 8):
        zp[rim, at:at + 8, :] = jnp.where(lane < LANES // 2, zp[1, at:at + 8, :], zp[blocks, at:at + 8, :])
    loop(0, groups + 1, lambda g: first_pass(g, [outside, edges]))
    loop(0, 2, lambda i: first_pass(i * groups, own))
    loop(0, 2, lambda i: second_pass(i * (groups - 1), own, keep))
    loop(0, groups, lambda g: second_pass(g, [edges], keep_edges))

    half = LANES // 2

    def window(field):
        def beside(right, left):
            a, b = srecv[right, 0:crows, :], srecv[left, 0:crows, :]
            return jnp.where(lane_c < half, a, b) if field == 0 else pltpu.roll(jnp.where(lane_c < half, b, a), half, 1)

        at = slice(field * crows, (field + 1) * crows)
        here = jnp.concatenate([coarse[at, :], beside(0, 4)], axis=1)
        below = jnp.concatenate([vrecv[0, at, :], beside(1, 3)], axis=1)
        above = jnp.concatenate([vrecv[1, at, :], beside(7, 5)], axis=1)
        sub_w = lax.broadcasted_iota(jnp.int32, (8, 2 * LANES), 0)
        mixed = jnp.where(sub_w < 4, below[8:16], above[crows - 16:crows - 8])
        return jnp.concatenate([here, below[0:8], mixed, above[crows - 8:crows]], axis=0)

    z = window(0)
    supply = window(1)
    high = z.shape[0]

    def turn(x, step, axis):
        return x if step == 0 else pltpu.roll(x, (-step) % x.shape[axis], axis)

    turned = {step: turn(z, step, 1) for step in (-1, 0, 1)}
    slopes = []
    for k, (step_row, step_col) in enumerate(OFFSETS):
        slopes.append(coef[k] * jnp.maximum(z - turn(turned[step_col], step_row, 0), 0.0))
    share = 1.0 / (functools.reduce(jnp.add, slopes) + RETENTION)
    weight = {}
    for k, (step_row, step_col) in enumerate(OFFSETS):
        weight[step_row, step_col] = turn(slopes[k] * share, -step_col, 1)
    flow = supply
    for _ in range(ITERS):
        moved = {step: turn(flow, -step, 1) for step in (-1, 0, 1)}
        sums = {}
        for step_row in (-1, 0, 1):
            sums[step_row] = functools.reduce(
                jnp.add, [weight[step_row, c] * moved[c] for c in (-1, 0, 1) if (step_row, c) in weight])
        flow = supply + sums[0] + turn(sums[1], -1, 0) + turn(sums[-1], 1, 0)

    left = turn(flow, -1, 1)[:, :LANES]
    right = turn(flow, 1, 1)[:, :LANES]
    centre = flow[:, :LANES]
    first, last = (lane & 7) == 0, (lane & 7) == 7
    per_block = LANES // 8
    for j in range(blocks):
        index = lane // 8 + j * per_block
        spread = []
        for at in list(range(0, crows, 8)) + [crows, high - 8]:
            mid = take_lanes(centre[at:at + 8], index)
            beside = jnp.where(first, take_lanes(left[at:at + 8], index), take_lanes(right[at:at + 8], index))
            spread.append((mid, beside))
        for g in range(groups):
            def level(number, group):
                where_at = {-1: (len(spread) - 1, 7), groups: (len(spread) - 2, 0)}.get(group, (group // 8, group % 8))
                line = spread[where_at[0]][number][where_at[1]:where_at[1] + 1, :]
                return jnp.broadcast_to(line, (8, LANES))

            at = slice(8 * g, 8 * g + 8)
            value = mask[j, at, :].astype(F32)
            for number in range(2):
                value = value + parts[number, j, at, :] * level(number, g)
                across = jnp.where(sub == 0, level(number, g - 1), level(number, g + 1))
                value = value + parts[2 + number, j, at, :] * across
            out_ref[at, j * LANES:(j + 1) * LANES] = value

    for k in range(8):
        @pl.when(exists[k])
        def _():
            for copy in copies(k):
                copy.wait_send()


def solution(mesh):
    row_devices, col_devices = mesh.shape["rows"], mesh.shape["cols"]

    def on_device(elevation, data_mask, tie_order):
        rows, cols = elevation.shape
        groups, blocks = rows // 8, cols // LANES
        return pl.pallas_call(
            functools.partial(kernel, row_devices, col_devices),
            out_shape=jax.ShapeDtypeStruct((rows, cols), F32),
            in_specs=[pl.BlockSpec(memory_space=pl.ANY)] * 3,
            out_specs=pl.BlockSpec(memory_space=pltpu.VMEM),
            scratch_shapes=[
                pltpu.SMEM((8,), jnp.int32),
                pltpu.VMEM((blocks + 2, rows + 16, LANES), F32),
                pltpu.VMEM((blocks, rows, LANES), jnp.int32),
                pltpu.VMEM((blocks + 2, rows + 16, LANES), F32),
                pltpu.VMEM((4, blocks, rows, LANES), F32),
                pltpu.VMEM((cols, LANES), jnp.bfloat16),
                pltpu.VMEM((2 * groups, LANES), F32),
                pltpu.VMEM((groups + 8, LANES), F32),
                pltpu.VMEM((8, groups + 8, LANES), F32),
                pltpu.VMEM((2, 2 * groups, LANES), F32),
                pltpu.SemaphoreType.DMA((2 * blocks,)),
                pltpu.SemaphoreType.DMA,
                pltpu.SemaphoreType.DMA((16,)),
                pltpu.SemaphoreType.DMA((16,)),
            ],
            compiler_params=pltpu.CompilerParams(collective_id=0, has_side_effects=True),
        )(tie_order, elevation, data_mask)

    return jax.shard_map(
        on_device, mesh=mesh, in_specs=(P("rows", "cols"), P("rows", "cols"), P()),
        out_specs=P("rows", "cols"), check_vma=False)
```

```python
import functools

import jax
import jax.numpy as jnp
from jax import lax
from jax.experimental import pallas as pl
from jax.experimental.pallas import tpu as pltpu
from jax.sharding import PartitionSpec as P

ITERS = 8
OFFSETS = ((0, 1), (1, 1), (1, 0), (1, -1), (0, -1), (-1, -1), (-1, 0), (-1, 1))
RECIPROCAL = (1.0, 0.7071067811865476) * 4
RETENTION = 0.1
OUTSIDE = 1000.0
LANES = 128
F32 = jnp.float32


def coefficients(tie_ref):
    out = []
    for k in range(8):
        value = jnp.float32(0.0)
        for i in range(8):
            place = jnp.float32((1.0 + 0.5 * (7.0 - i) / 7.0) * RECIPROCAL[k])
            value = jnp.where(tie_ref[i] == k, place, value)
        out.append(value)
    return out


def shift_lanes(before, here, after, step, lane):
    if step == 0:
        return here
    if step < 0:
        return pltpu.roll(jnp.where(lane == LANES - 1, before, here), 1, 1)
    return pltpu.roll(jnp.where(lane == 0, after, here), LANES - 1, 1)


def take_lanes(values, index):
    return jnp.take_along_axis(values, index, axis=1, mode="promise_in_bounds")


def kernel(row_devices, col_devices, tie_hbm, elev_ref, mask_ref, out_ref, tie_ref, zp, zl, zr, mask, recip, rl, rr, parts, ones,
           coarse, side, srecv, vrecv, load_sem, tie_sem, send_sem, recv_sem):
    rows, cols = elev_ref.shape
    groups, blocks = rows // 8, cols // LANES
    crows = groups
    row, col = lax.axis_index("rows"), lax.axis_index("cols")
    ring, rim = 0, blocks + 1

    loads = []
    for j in range(blocks):
        part = pl.ds(j * LANES, LANES)
        loads.append((
            pltpu.make_async_copy(elev_ref.at[:, part], zp.at[j + 1, pl.ds(8, rows), :], load_sem.at[j]),
            pltpu.make_async_copy(mask_ref.at[:, part], mask.at[j], load_sem.at[blocks + j])))
        loads[-1][0].start()
        loads[-1][1].start()
    tie_load = pltpu.make_async_copy(tie_hbm, tie_ref, tie_sem)
    tie_load.start()

    barrier = pltpu.get_barrier_semaphore()
    exists = []
    for step_row, step_col in OFFSETS:
        there = jnp.bool_(True)
        if step_row > 0:
            there = row < row_devices - 1
        if step_row < 0:
            there = row > 0
        if step_col > 0:
            there = jnp.logical_and(there, col < col_devices - 1)
        if step_col < 0:
            there = jnp.logical_and(there, col > 0)
        exists.append(there)

    def peer(k):
        return {"rows": row + OFFSETS[k][0], "cols": col + OFFSETS[k][1]}

    for k in range(8):
        @pl.when(exists[k])
        def _():
            pl.semaphore_signal(barrier, inc=1, device_id=peer(k), device_id_type=pl.DeviceIdType.MESH)

    lane = lax.broadcasted_iota(jnp.int32, (8, LANES), 1)
    sub = lax.broadcasted_iota(jnp.int32, (8, LANES), 0)
    lane_c = lax.broadcasted_iota(jnp.int32, (crows, LANES), 1)
    middle_lanes = jnp.logical_and(lane_c >= LANES // 4, lane_c < 3 * LANES // 4)

    SIDES, UPDOWN = (0, 1, 3, 4, 5, 7), (2, 6)

    def halo_rows(k):
        return zp.at[pl.ds(1, blocks), pl.ds(8 + rows if k == 2 else 0, 8), :]

    def edge_rows(k):
        return zp.at[pl.ds(1, blocks), pl.ds(rows if k == 2 else 8, 8), :]

    for k in range(8):
        @pl.when(jnp.logical_not(exists[k]))
        def _():
            if k in UPDOWN:
                region = halo_rows(k)
                region[...] = jnp.full(region.shape, OUTSIDE, F32)
                vrecv[k // 4, 0:crows, :] = jnp.full((crows, LANES), OUTSIDE, F32)
                vrecv[k // 4, crows:2 * crows, :] = jnp.zeros((crows, LANES), F32)
            else:
                srecv[k, 0:crows, :] = jnp.where(middle_lanes, 0.0, OUTSIDE)
                srecv[k, crows:crows + 8, :] = jnp.full((8, LANES), OUTSIDE, F32)

    ones[...] = (
        lax.broadcasted_iota(jnp.int32, (cols, LANES), 0) // 8 == lax.broadcasted_iota(jnp.int32, (cols, LANES), 1)
    ).astype(F32).astype(jnp.bfloat16)

    total = jnp.zeros((4 * crows, LANES), F32)
    for j in range(blocks):
        loads[j][0].wait()
        loads[j][1].wait()
        height_sum = jnp.zeros((crows, LANES), F32)
        count_sum = jnp.zeros((crows, LANES), F32)
        for s in range(8):
            valid = mask[j, pl.ds(s, crows, stride=8), :].astype(F32)
            height_sum = height_sum + valid * zp[j + 1, pl.ds(8 + s, crows, stride=8), :]
            count_sum = count_sum + valid
        high = height_sum.astype(jnp.bfloat16)
        rest = height_sum - high.astype(F32)
        middle = rest.astype(jnp.bfloat16)
        low = (rest - middle.astype(F32)).astype(jnp.bfloat16)
        stacked = jnp.concatenate([count_sum.astype(jnp.bfloat16), high, middle, low], axis=0)
        total = total + jnp.dot(stacked, ones[j * LANES:(j + 1) * LANES, :], preferred_element_type=F32)
    counts = total[0:crows]
    heights = total[crows:2 * crows] + (total[2 * crows:3 * crows] + total[3 * crows:])
    overview = heights / (counts + 1.0)
    runoff = counts * (1.0 / 64.0)

    packed = jnp.zeros((8, LANES), F32)
    for g in range(groups):
        at = pl.ds(8 + 8 * g, 8)
        edges = jnp.where(lane < LANES // 2, zp[1, at, :], zp[blocks, at, :])
        zp[rim, at, :] = edges
        packed = jnp.where(lane // 4 == g, pltpu.roll(edges, (2 + 4 * g) % LANES, 1), packed)
    side[crows:crows + 8, :] = packed
    side[0:crows, :] = jnp.where(middle_lanes, pltpu.roll(runoff, LANES // 2, 1), overview)
    coarse[0:crows, :] = overview
    coarse[crows:2 * crows, :] = runoff

    pl.semaphore_wait(barrier, functools.reduce(jnp.add, [there.astype(jnp.int32) for there in exists]))

    def copies(k, arriving=False):
        slot = k if arriving else (k + 4) % 8

        def remote(src, dst, extra):
            return pltpu.make_async_remote_copy(
                src_ref=src, dst_ref=dst, send_sem=send_sem.at[k + extra], recv_sem=recv_sem.at[slot + extra],
                device_id=peer(k), device_id_type=pl.DeviceIdType.MESH)

        if k in UPDOWN:
            return [remote(coarse, vrecv.at[slot // 4], 0), remote(edge_rows(k), halo_rows(slot), 8)]
        return [remote(side, srecv.at[slot], 0)]

    for k in (1, 3, 5, 7, 0, 4, 2, 6):
        @pl.when(exists[k])
        def _():
            for copy in copies(k):
                copy.start()

    tie_load.wait()
    coef = coefficients(tie_ref)

    def beside_heights(at, around):
        for j, before, after in around:
            line = [zp[b, at, :] for b in (before, j, after)]
            zl[j, at, :] = shift_lanes(*line, -1, lane)
            zr[j, at, :] = shift_lanes(*line, 1, lane)

    by_column = {-1: zl, 0: zp, 1: zr}
    scale_by_column = {-1: rl, 0: recip, 1: rr}

    def first_pass(g, around):
        done = {}
        middle_at = pl.ds(8 * g + 7, 8)
        for j, before, after in around:
            here = zp[j, middle_at, :]
            summed = jnp.full((8, LANES), RETENTION, F32)
            for k, (off_row, off_col) in enumerate(OFFSETS):
                beside = by_column[off_col][j, pl.ds(8 * g + 7 + off_row, 8), :]
                summed = summed + coef[k] * jnp.maximum(here - beside, 0.0)
            done[j] = 1.0 / summed
            recip[j, middle_at, :] = done[j]
        for j, before, after in around:
            line = [done.get(b, done[j]) for b in (before, j, after)]
            rl[j, middle_at, :] = shift_lanes(*line, -1, lane)
            rr[j, middle_at, :] = shift_lanes(*line, 1, lane)

    def second_pass(g, around, store):
        for j, before, after in around:
            here = zp[j, pl.ds(8 * g + 8, 8), :]
            inside, outer = {}, {}
            for step_col in (-1, 0, 1):
                terms = {}
                for step_row in (-1, 0, 1):
                    if (step_row, step_col) == (0, 0):
                        continue
                    k = OFFSETS.index((-step_row, -step_col))
                    at = pl.ds(8 * g + 8 + step_row, 8)
                    source = by_column[step_col][j, at, :]
                    scale = scale_by_column[step_col][j, at, :]
                    terms[step_row] = coef[k] * jnp.maximum(source - here, 0.0) * scale
                inside[step_col] = jnp.where(sub == 0, 0.0, terms[-1]) + jnp.where(sub == 7, 0.0, terms[1])
                if step_col != 0:
                    inside[step_col] = inside[step_col] + terms[0]
                outer[step_col] = jnp.where(sub == 0, terms[-1], jnp.where(sub == 7, terms[1], 0.0))
            first, last = (lane & 7) == 0, (lane & 7) == 7
            for number, field in enumerate((inside, outer)):
                store(g, j, 2 * number, field[0] + jnp.where(first, 0.0, field[-1]) + jnp.where(last, 0.0, field[1]))
                store(g, j, 2 * number + 1, jnp.where(first, field[-1], jnp.where(last, field[1], 0.0)))

    def keep(g, j, number, value):
        parts[number, j - 1, pl.ds(8 * g, 8), :] = value

    def keep_edges(g, j, number, value):
        at = pl.ds(8 * g, 8)
        parts[number, 0, at, :] = jnp.where(lane < 8, value, parts[number, 0, at, :])
        parts[number, blocks - 1, at, :] = jnp.where(lane >= LANES - 8, value, parts[number, blocks - 1, at, :])

    own = [(j, j - 1, j + 1 if j < blocks else ring) for j in range(1, blocks + 1)]
    outside, edges = (ring, blocks, 1), (rim, ring, ring)

    def loop(start, stop, body):
        def step(g, carry):
            body(g)
            return carry

        lax.fori_loop(start, stop, step, 0)

    loop(0, groups, lambda g: beside_heights(pl.ds(pl.multiple_of(8 * g + 8, 8), 8), own))
    loop(1, groups, lambda g: first_pass(g, own))
    loop(1, groups - 1, lambda g: second_pass(g, own, keep))

    for k in range(8):
        @pl.when(exists[k])
        def _():
            for copy in copies(k, arriving=True):
                copy.wait_recv()

    def outside_columns(g, right, left):
        chosen = jnp.where(lane >= 4 * g + 2, srecv[right, crows:crows + 8, :], srecv[left, crows:crows + 8, :])
        return pltpu.roll(chosen, (2 * LANES - 4 * g - 2) % LANES, 1)

    for g in range(groups):
        zp[ring, pl.ds(8 + 8 * g, 8), :] = outside_columns(g, 0, 4)
    zp[ring, 0:8, :] = outside_columns(groups - 1, 7, 5)
    zp[ring, rows + 8:rows + 16, :] = outside_columns(0, 1, 3)
    for at in (0, rows + 8):
        zp[rim, at:at + 8, :] = jnp.where(lane < LANES // 2, zp[1, at:at + 8, :], zp[blocks, at:at + 8, :])
    for at in (0, rows + 8):
        beside_heights(pl.ds(at, 8), own)
    loop(0, groups + 2, lambda g: beside_heights(pl.ds(pl.multiple_of(8 * g, 8), 8), [outside, edges]))
    loop(0, groups + 1, lambda g: first_pass(g, [outside, edges]))
    loop(0, 2, lambda i: first_pass(i * groups, own))
    loop(0, 2, lambda i: second_pass(i * (groups - 1), own, keep))
    loop(0, groups, lambda g: second_pass(g, [edges], keep_edges))

    half = LANES // 2

    def window(field):
        def beside(right, left):
            a, b = srecv[right, 0:crows, :], srecv[left, 0:crows, :]
            return jnp.where(lane_c < half, a, b) if field == 0 else pltpu.roll(jnp.where(lane_c < half, b, a), half, 1)

        at = slice(field * crows, (field + 1) * crows)
        here = jnp.concatenate([coarse[at, :], beside(0, 4)], axis=1)
        below = jnp.concatenate([vrecv[0, at, :], beside(1, 3)], axis=1)
        above = jnp.concatenate([vrecv[1, at, :], beside(7, 5)], axis=1)
        sub_w = lax.broadcasted_iota(jnp.int32, (8, 2 * LANES), 0)
        mixed = jnp.where(sub_w < 4, below[8:16], above[crows - 16:crows - 8])
        return jnp.concatenate([here, below[0:8], mixed, above[crows - 8:crows]], axis=0)

    z = window(0)
    supply = window(1)
    high = z.shape[0]

    def turn(x, step, axis):
        return x if step == 0 else pltpu.roll(x, (-step) % x.shape[axis], axis)

    turned = {step: turn(z, step, 1) for step in (-1, 0, 1)}
    slopes = []
    for k, (step_row, step_col) in enumerate(OFFSETS):
        slopes.append(coef[k] * jnp.maximum(z - turn(turned[step_col], step_row, 0), 0.0))
    share = 1.0 / (functools.reduce(jnp.add, slopes) + RETENTION)
    weight = {}
    for k, (step_row, step_col) in enumerate(OFFSETS):
        weight[step_row, step_col] = turn(slopes[k] * share, -step_col, 1)
    flow = supply
    for _ in range(ITERS):
        moved = {step: turn(flow, -step, 1) for step in (-1, 0, 1)}
        sums = {}
        for step_row in (-1, 0, 1):
            sums[step_row] = functools.reduce(
                jnp.add, [weight[step_row, c] * moved[c] for c in (-1, 0, 1) if (step_row, c) in weight])
        flow = supply + sums[0] + turn(sums[1], -1, 0) + turn(sums[-1], 1, 0)

    left = turn(flow, -1, 1)[:, :LANES]
    right = turn(flow, 1, 1)[:, :LANES]
    centre = flow[:, :LANES]
    first, last = (lane & 7) == 0, (lane & 7) == 7
    per_block = LANES // 8
    for j in range(blocks):
        index = lane // 8 + j * per_block
        spread = []
        for at in list(range(0, crows, 8)) + [crows, high - 8]:
            mid = take_lanes(centre[at:at + 8], index)
            beside = jnp.where(first, take_lanes(left[at:at + 8], index), take_lanes(right[at:at + 8], index))
            spread.append((mid, beside))
        for g in range(groups):
            def level(number, group):
                where_at = {-1: (len(spread) - 1, 7), groups: (len(spread) - 2, 0)}.get(group, (group // 8, group % 8))
                line = spread[where_at[0]][number][where_at[1]:where_at[1] + 1, :]
                return jnp.broadcast_to(line, (8, LANES))

            at = slice(8 * g, 8 * g + 8)
            value = mask[j, at, :].astype(F32)
            for number in range(2):
                value = value + parts[number, j, at, :] * level(number, g)
                across = jnp.where(sub == 0, level(number, g - 1), level(number, g + 1))
                value = value + parts[2 + number, j, at, :] * across
            out_ref[at, j * LANES:(j + 1) * LANES] = value

    for k in range(8):
        @pl.when(exists[k])
        def _():
            for copy in copies(k):
                copy.wait_send()


def solution(mesh):
    row_devices, col_devices = mesh.shape["rows"], mesh.shape["cols"]

    def on_device(elevation, data_mask, tie_order):
        rows, cols = elevation.shape
        groups, blocks = rows // 8, cols // LANES
        return pl.pallas_call(
            functools.partial(kernel, row_devices, col_devices),
            out_shape=jax.ShapeDtypeStruct((rows, cols), F32),
            in_specs=[pl.BlockSpec(memory_space=pl.ANY)] * 3,
            out_specs=pl.BlockSpec(memory_space=pltpu.VMEM),
            scratch_shapes=[
                pltpu.SMEM((8,), jnp.int32),
                pltpu.VMEM((blocks + 2, rows + 16, LANES), F32),
                pltpu.VMEM((blocks + 2, rows + 16, LANES), F32),
                pltpu.VMEM((blocks + 2, rows + 16, LANES), F32),
                pltpu.VMEM((blocks, rows, LANES), jnp.int32),
                pltpu.VMEM((blocks + 2, rows + 16, LANES), F32),
                pltpu.VMEM((blocks + 2, rows + 16, LANES), F32),
                pltpu.VMEM((blocks + 2, rows + 16, LANES), F32),
                pltpu.VMEM((4, blocks, rows, LANES), F32),
                pltpu.VMEM((cols, LANES), jnp.bfloat16),
                pltpu.VMEM((2 * groups, LANES), F32),
                pltpu.VMEM((groups + 8, LANES), F32),
                pltpu.VMEM((8, groups + 8, LANES), F32),
                pltpu.VMEM((2, 2 * groups, LANES), F32),
                pltpu.SemaphoreType.DMA((2 * blocks,)),
                pltpu.SemaphoreType.DMA,
                pltpu.SemaphoreType.DMA((16,)),
                pltpu.SemaphoreType.DMA((16,)),
            ],
            compiler_params=pltpu.CompilerParams(collective_id=0, has_side_effects=True),
        )(tie_order, elevation, data_mask)

    return jax.shard_map(
        on_device, mesh=mesh, in_specs=(P("rows", "cols"), P("rows", "cols"), P()),
        out_specs=P("rows", "cols"), check_vma=False)
```

```python
import functools

import jax
import jax.numpy as jnp
from jax import lax
from jax.experimental import pallas as pl
from jax.experimental.pallas import tpu as pltpu
from jax.sharding import PartitionSpec as P

ITERS = 8
OFFSETS = ((0, 1), (1, 1), (1, 0), (1, -1), (0, -1), (-1, -1), (-1, 0), (-1, 1))
RECIPROCAL = (1.0, 0.7071067811865476) * 4
RETENTION = 0.1
OUTSIDE = 1000.0
LANES = 128
F32 = jnp.float32


def coefficients(tie_ref):
    out = []
    for k in range(8):
        value = jnp.float32(0.0)
        for i in range(8):
            place = jnp.float32((1.0 + 0.5 * (7.0 - i) / 7.0) * RECIPROCAL[k])
            value = jnp.where(tie_ref[i] == k, place, value)
        out.append(value)
    return out


def shift_lanes(before, here, after, step, lane):
    if step == 0:
        return here
    if step < 0:
        return pltpu.roll(jnp.where(lane == LANES - 1, before, here), 1, 1)
    return pltpu.roll(jnp.where(lane == 0, after, here), LANES - 1, 1)


def take_lanes(values, index):
    return jnp.take_along_axis(values, index, axis=1, mode="promise_in_bounds")


def kernel(row_devices, col_devices, tie_hbm, elev_ref, mask_ref, out_ref, tie_ref, zp, zl, zr, mask, recip, rl, rr, parts, ones,
           coarse, side, srecv, vrecv, load_sem, tie_sem, send_sem, recv_sem):
    rows, cols = elev_ref.shape
    groups, blocks = rows // 8, cols // LANES
    crows = groups
    row, col = lax.axis_index("rows"), lax.axis_index("cols")
    ring, rim = 0, blocks + 1

    loads = []
    for j in range(blocks):
        part = pl.ds(j * LANES, LANES)
        loads.append((
            pltpu.make_async_copy(elev_ref.at[:, part], zp.at[j + 1, pl.ds(8, rows), :], load_sem.at[j]),
            pltpu.make_async_copy(mask_ref.at[:, part], mask.at[j], load_sem.at[blocks + j])))
        loads[-1][0].start()
        loads[-1][1].start()
    tie_load = pltpu.make_async_copy(tie_hbm, tie_ref, tie_sem)
    tie_load.start()

    barrier = pltpu.get_barrier_semaphore()
    exists = []
    for step_row, step_col in OFFSETS:
        there = jnp.bool_(True)
        if step_row > 0:
            there = row < row_devices - 1
        if step_row < 0:
            there = row > 0
        if step_col > 0:
            there = jnp.logical_and(there, col < col_devices - 1)
        if step_col < 0:
            there = jnp.logical_and(there, col > 0)
        exists.append(there)

    def peer(k):
        return {"rows": row + OFFSETS[k][0], "cols": col + OFFSETS[k][1]}

    for k in range(8):
        @pl.when(exists[k])
        def _():
            pl.semaphore_signal(barrier, inc=1, device_id=peer(k), device_id_type=pl.DeviceIdType.MESH)

    lane = lax.broadcasted_iota(jnp.int32, (8, LANES), 1)
    sub = lax.broadcasted_iota(jnp.int32, (8, LANES), 0)
    lane_c = lax.broadcasted_iota(jnp.int32, (crows, LANES), 1)
    middle_lanes = jnp.logical_and(lane_c >= LANES // 4, lane_c < 3 * LANES // 4)

    SIDES, UPDOWN = (0, 1, 3, 4, 5, 7), (2, 6)

    def halo_rows(k):
        return zp.at[pl.ds(1, blocks), pl.ds(8 + rows if k == 2 else 0, 8), :]

    def edge_rows(k):
        return zp.at[pl.ds(1, blocks), pl.ds(rows if k == 2 else 8, 8), :]

    for k in range(8):
        @pl.when(jnp.logical_not(exists[k]))
        def _():
            if k in UPDOWN:
                region = halo_rows(k)
                region[...] = jnp.full(region.shape, OUTSIDE, F32)
                vrecv[k // 4, 0:crows, :] = jnp.full((crows, LANES), OUTSIDE, F32)
                vrecv[k // 4, crows:2 * crows, :] = jnp.zeros((crows, LANES), F32)
            else:
                srecv[k, 0:crows, :] = jnp.where(middle_lanes, 0.0, OUTSIDE)
                srecv[k, crows:crows + 8, :] = jnp.full((8, LANES), OUTSIDE, F32)

    ones[...] = (
        lax.broadcasted_iota(jnp.int32, (cols, LANES), 0) // 8 == lax.broadcasted_iota(jnp.int32, (cols, LANES), 1)
    ).astype(F32).astype(jnp.bfloat16)

    total = jnp.zeros((4 * crows, LANES), F32)
    for j in range(blocks):
        loads[j][0].wait()
        loads[j][1].wait()
        height_sum = jnp.zeros((crows, LANES), F32)
        count_sum = jnp.zeros((crows, LANES), F32)
        for s in range(8):
            valid = mask[j, pl.ds(s, crows, stride=8), :].astype(F32)
            height_sum = height_sum + valid * zp[j + 1, pl.ds(8 + s, crows, stride=8), :]
            count_sum = count_sum + valid
        high = height_sum.astype(jnp.bfloat16)
        rest = height_sum - high.astype(F32)
        middle = rest.astype(jnp.bfloat16)
        low = (rest - middle.astype(F32)).astype(jnp.bfloat16)
        stacked = jnp.concatenate([count_sum.astype(jnp.bfloat16), high, middle, low], axis=0)
        total = total + jnp.dot(stacked, ones[j * LANES:(j + 1) * LANES, :], preferred_element_type=F32)
    counts = total[0:crows]
    heights = total[crows:2 * crows] + (total[2 * crows:3 * crows] + total[3 * crows:])
    overview = heights / (counts + 1.0)
    runoff = counts * (1.0 / 64.0)

    packed = jnp.zeros((8, LANES), F32)
    for g in range(groups):
        at = pl.ds(8 + 8 * g, 8)
        edges = jnp.where(lane < LANES // 2, zp[1, at, :], zp[blocks, at, :])
        zp[rim, at, :] = edges
        packed = jnp.where(lane // 4 == g, pltpu.roll(edges, (2 + 4 * g) % LANES, 1), packed)
    side[crows:crows + 8, :] = packed
    side[0:crows, :] = jnp.where(middle_lanes, pltpu.roll(runoff, LANES // 2, 1), overview)
    coarse[0:crows, :] = overview
    coarse[crows:2 * crows, :] = runoff

    pl.semaphore_wait(barrier, functools.reduce(jnp.add, [there.astype(jnp.int32) for there in exists]))

    def copies(k, arriving=False):
        slot = k if arriving else (k + 4) % 8

        def remote(src, dst, extra):
            return pltpu.make_async_remote_copy(
                src_ref=src, dst_ref=dst, send_sem=send_sem.at[k + extra], recv_sem=recv_sem.at[slot + extra],
                device_id=peer(k), device_id_type=pl.DeviceIdType.MESH)

        if k in UPDOWN:
            return remote(edge_rows(k), halo_rows(slot), 8), remote(coarse, vrecv.at[slot // 4], 0)
        fine, wide = pl.ds(crows, 8), pl.ds(0, crows)
        return (remote(side.at[fine, :], srecv.at[slot, fine, :], 8),
                remote(side.at[wide, :], srecv.at[slot, wide, :], 0))

    for which in range(2):
        for k in (1, 3, 5, 7, 0, 4, 2, 6):
            @pl.when(exists[k])
            def _():
                copies(k)[which].start()

    tie_load.wait()
    coef = coefficients(tie_ref)

    def beside_heights(at, around):
        for j, before, after in around:
            line = [zp[b, at, :] for b in (before, j, after)]
            zl[j, at, :] = shift_lanes(*line, -1, lane)
            zr[j, at, :] = shift_lanes(*line, 1, lane)

    by_column = {-1: zl, 0: zp, 1: zr}
    scale_by_column = {-1: rl, 0: recip, 1: rr}

    def first_pass(g, around):
        done = {}
        middle_at = pl.ds(8 * g + 7, 8)
        for j, before, after in around:
            here = zp[j, middle_at, :]
            summed = jnp.full((8, LANES), RETENTION, F32)
            for k, (off_row, off_col) in enumerate(OFFSETS):
                beside = by_column[off_col][j, pl.ds(8 * g + 7 + off_row, 8), :]
                summed = summed + coef[k] * jnp.maximum(here - beside, 0.0)
            done[j] = 1.0 / summed
            recip[j, middle_at, :] = done[j]
        for j, before, after in around:
            line = [done.get(b, done[j]) for b in (before, j, after)]
            rl[j, middle_at, :] = shift_lanes(*line, -1, lane)
            rr[j, middle_at, :] = shift_lanes(*line, 1, lane)

    def second_pass(g, around, store):
        for j, before, after in around:
            here = zp[j, pl.ds(8 * g + 8, 8), :]
            inside, outer = {}, {}
            for step_col in (-1, 0, 1):
                terms = {}
                for step_row in (-1, 0, 1):
                    if (step_row, step_col) == (0, 0):
                        continue
                    k = OFFSETS.index((-step_row, -step_col))
                    at = pl.ds(8 * g + 8 + step_row, 8)
                    source = by_column[step_col][j, at, :]
                    scale = scale_by_column[step_col][j, at, :]
                    terms[step_row] = coef[k] * jnp.maximum(source - here, 0.0) * scale
                inside[step_col] = jnp.where(sub == 0, 0.0, terms[-1]) + jnp.where(sub == 7, 0.0, terms[1])
                if step_col != 0:
                    inside[step_col] = inside[step_col] + terms[0]
                outer[step_col] = jnp.where(sub == 0, terms[-1], jnp.where(sub == 7, terms[1], 0.0))
            first, last = (lane & 7) == 0, (lane & 7) == 7
            for number, field in enumerate((inside, outer)):
                store(g, j, 2 * number, field[0] + jnp.where(first, 0.0, field[-1]) + jnp.where(last, 0.0, field[1]))
                store(g, j, 2 * number + 1, jnp.where(first, field[-1], jnp.where(last, field[1], 0.0)))

    def keep(g, j, number, value):
        parts[number, j - 1, pl.ds(8 * g, 8), :] = value

    def keep_edges(g, j, number, value):
        at = pl.ds(8 * g, 8)
        parts[number, 0, at, :] = jnp.where(lane < 8, value, parts[number, 0, at, :])
        parts[number, blocks - 1, at, :] = jnp.where(lane >= LANES - 8, value, parts[number, blocks - 1, at, :])

    own = [(j, j - 1, j + 1 if j < blocks else ring) for j in range(1, blocks + 1)]
    outside, edges = (ring, blocks, 1), (rim, ring, ring)

    def loop(start, stop, body):
        def step(g, carry):
            body(g)
            return carry

        lax.fori_loop(start, stop, step, 0)

    loop(0, groups, lambda g: beside_heights(pl.ds(pl.multiple_of(8 * g + 8, 8), 8), own))
    loop(1, groups, lambda g: first_pass(g, own))
    loop(1, groups - 1, lambda g: second_pass(g, own, keep))

    def receive(which):
        for k in range(8):
            @pl.when(exists[k])
            def _():
                copies(k, arriving=True)[which].wait_recv()

    receive(0)

    def outside_columns(g, right, left):
        chosen = jnp.where(lane >= 4 * g + 2, srecv[right, crows:crows + 8, :], srecv[left, crows:crows + 8, :])
        return pltpu.roll(chosen, (2 * LANES - 4 * g - 2) % LANES, 1)

    for g in range(groups):
        zp[ring, pl.ds(8 + 8 * g, 8), :] = outside_columns(g, 0, 4)
    zp[ring, 0:8, :] = outside_columns(groups - 1, 7, 5)
    zp[ring, rows + 8:rows + 16, :] = outside_columns(0, 1, 3)
    for at in (0, rows + 8):
        zp[rim, at:at + 8, :] = jnp.where(lane < LANES // 2, zp[1, at:at + 8, :], zp[blocks, at:at + 8, :])
    for at in (0, rows + 8):
        beside_heights(pl.ds(at, 8), own)
    loop(0, groups + 2, lambda g: beside_heights(pl.ds(pl.multiple_of(8 * g, 8), 8), [outside, edges]))
    loop(0, groups + 1, lambda g: first_pass(g, [outside, edges]))
    loop(0, 2, lambda i: first_pass(i * groups, own))
    loop(0, 2, lambda i: second_pass(i * (groups - 1), own, keep))
    loop(0, groups, lambda g: second_pass(g, [edges], keep_edges))

    receive(1)

    half = LANES // 2

    def window(field):
        def beside(right, left):
            a, b = srecv[right, 0:crows, :], srecv[left, 0:crows, :]
            return jnp.where(lane_c < half, a, b) if field == 0 else pltpu.roll(jnp.where(lane_c < half, b, a), half, 1)

        at = slice(field * crows, (field + 1) * crows)
        here = jnp.concatenate([coarse[at, :], beside(0, 4)], axis=1)
        below = jnp.concatenate([vrecv[0, at, :], beside(1, 3)], axis=1)
        above = jnp.concatenate([vrecv[1, at, :], beside(7, 5)], axis=1)
        sub_w = lax.broadcasted_iota(jnp.int32, (8, 2 * LANES), 0)
        mixed = jnp.where(sub_w < 4, below[8:16], above[crows - 16:crows - 8])
        return jnp.concatenate([here, below[0:8], mixed, above[crows - 8:crows]], axis=0)

    z = window(0)
    supply = window(1)
    high = z.shape[0]

    def turn(x, step, axis):
        return x if step == 0 else pltpu.roll(x, (-step) % x.shape[axis], axis)

    turned = {step: turn(z, step, 1) for step in (-1, 0, 1)}
    slopes = []
    for k, (step_row, step_col) in enumerate(OFFSETS):
        slopes.append(coef[k] * jnp.maximum(z - turn(turned[step_col], step_row, 0), 0.0))
    share = 1.0 / (functools.reduce(jnp.add, slopes) + RETENTION)
    weight = {}
    for k, (step_row, step_col) in enumerate(OFFSETS):
        weight[step_row, step_col] = turn(slopes[k] * share, -step_col, 1)
    flow = supply
    for _ in range(ITERS):
        moved = {step: turn(flow, -step, 1) for step in (-1, 0, 1)}
        sums = {}
        for step_row in (-1, 0, 1):
            sums[step_row] = functools.reduce(
                jnp.add, [weight[step_row, c] * moved[c] for c in (-1, 0, 1) if (step_row, c) in weight])
        flow = supply + sums[0] + turn(sums[1], -1, 0) + turn(sums[-1], 1, 0)

    left = turn(flow, -1, 1)[:, :LANES]
    right = turn(flow, 1, 1)[:, :LANES]
    centre = flow[:, :LANES]
    first, last = (lane & 7) == 0, (lane & 7) == 7
    per_block = LANES // 8
    for j in range(blocks):
        index = lane // 8 + j * per_block
        spread = []
        for at in list(range(0, crows, 8)) + [crows, high - 8]:
            mid = take_lanes(centre[at:at + 8], index)
            beside = jnp.where(first, take_lanes(left[at:at + 8], index), take_lanes(right[at:at + 8], index))
            spread.append((mid, beside))
        for g in range(groups):
            def level(number, group):
                where_at = {-1: (len(spread) - 1, 7), groups: (len(spread) - 2, 0)}.get(group, (group // 8, group % 8))
                line = spread[where_at[0]][number][where_at[1]:where_at[1] + 1, :]
                return jnp.broadcast_to(line, (8, LANES))

            at = slice(8 * g, 8 * g + 8)
            value = mask[j, at, :].astype(F32)
            for number in range(2):
                value = value + parts[number, j, at, :] * level(number, g)
                across = jnp.where(sub == 0, level(number, g - 1), level(number, g + 1))
                value = value + parts[2 + number, j, at, :] * across
            out_ref[at, j * LANES:(j + 1) * LANES] = value

    for k in range(8):
        @pl.when(exists[k])
        def _():
            for copy in copies(k):
                copy.wait_send()


def solution(mesh):
    row_devices, col_devices = mesh.shape["rows"], mesh.shape["cols"]

    def on_device(elevation, data_mask, tie_order):
        rows, cols = elevation.shape
        groups, blocks = rows // 8, cols // LANES
        return pl.pallas_call(
            functools.partial(kernel, row_devices, col_devices),
            out_shape=pltpu.VMEM((rows, cols), F32),
            in_specs=[pl.BlockSpec(memory_space=pl.ANY)] * 3,
            out_specs=pl.BlockSpec(memory_space=pltpu.VMEM),
            scratch_shapes=[
                pltpu.SMEM((8,), jnp.int32),
                pltpu.VMEM((blocks + 2, rows + 16, LANES), F32),
                pltpu.VMEM((blocks + 2, rows + 16, LANES), F32),
                pltpu.VMEM((blocks + 2, rows + 16, LANES), F32),
                pltpu.VMEM((blocks, rows, LANES), jnp.int32),
                pltpu.VMEM((blocks + 2, rows + 16, LANES), F32),
                pltpu.VMEM((blocks + 2, rows + 16, LANES), F32),
                pltpu.VMEM((blocks + 2, rows + 16, LANES), F32),
                pltpu.VMEM((4, blocks, rows, LANES), F32),
                pltpu.VMEM((cols, LANES), jnp.bfloat16),
                pltpu.VMEM((2 * groups, LANES), F32),
                pltpu.VMEM((groups + 8, LANES), F32),
                pltpu.VMEM((8, groups + 8, LANES), F32),
                pltpu.VMEM((2, 2 * groups, LANES), F32),
                pltpu.SemaphoreType.DMA((2 * blocks,)),
                pltpu.SemaphoreType.DMA,
                pltpu.SemaphoreType.DMA((16,)),
                pltpu.SemaphoreType.DMA((16,)),
            ],
            compiler_params=pltpu.CompilerParams(collective_id=0, has_side_effects=True, vmem_limit_bytes=61000000),
        )(tie_order, elevation, data_mask)

    return jax.shard_map(
        on_device, mesh=mesh, in_specs=(P("rows", "cols"), P("rows", "cols"), P()),
        out_specs=P("rows", "cols"), check_vma=False)
```

```python
import functools

import jax
import jax.numpy as jnp
from jax import lax
from jax.experimental import pallas as pl
from jax.experimental.pallas import tpu as pltpu
from jax.sharding import PartitionSpec as P

ITERS = 8
OFFSETS = ((0, 1), (1, 1), (1, 0), (1, -1), (0, -1), (-1, -1), (-1, 0), (-1, 1))
RECIPROCAL = (1.0, 0.7071067811865476) * 4
RETENTION = 0.1
OUTSIDE = 1000.0
LANES = 128
F32 = jnp.float32


def coefficients(tie_ref):
    out = []
    for k in range(8):
        value = jnp.float32(0.0)
        for i in range(8):
            place = jnp.float32((1.0 + 0.5 * (7.0 - i) / 7.0) * RECIPROCAL[k])
            value = jnp.where(tie_ref[i] == k, place, value)
        out.append(value)
    return out


def shift_lanes(before, here, after, step, lane):
    if step == 0:
        return here
    if step < 0:
        return pltpu.roll(jnp.where(lane == LANES - 1, before, here), 1, 1)
    return pltpu.roll(jnp.where(lane == 0, after, here), LANES - 1, 1)


def take_lanes(values, index):
    return jnp.take_along_axis(values, index, axis=1, mode="promise_in_bounds")


def kernel(row_devices, col_devices, tie_hbm, elev_ref, mask_ref, out_ref, tie_ref, zp, zl, zr, mask, recip, rl, rr, parts, ones,
           coarse, side, srecv, vrecv, load_sem, tie_sem, send_sem, recv_sem):
    rows, cols = elev_ref.shape
    groups, blocks = rows // 8, cols // LANES
    crows = groups
    row, col = lax.axis_index("rows"), lax.axis_index("cols")
    ring, rim = 0, blocks + 1

    loads = []
    for j in range(blocks):
        part = pl.ds(j * LANES, LANES)
        loads.append((
            pltpu.make_async_copy(elev_ref.at[:, part], zp.at[j + 1, pl.ds(8, rows), :], load_sem.at[j]),
            pltpu.make_async_copy(mask_ref.at[:, part], mask.at[j], load_sem.at[blocks + j])))
        loads[-1][0].start()
        loads[-1][1].start()
    tie_load = pltpu.make_async_copy(tie_hbm, tie_ref, tie_sem)
    tie_load.start()

    barrier = pltpu.get_barrier_semaphore()
    exists = []
    for step_row, step_col in OFFSETS:
        there = jnp.bool_(True)
        if step_row > 0:
            there = row < row_devices - 1
        if step_row < 0:
            there = row > 0
        if step_col > 0:
            there = jnp.logical_and(there, col < col_devices - 1)
        if step_col < 0:
            there = jnp.logical_and(there, col > 0)
        exists.append(there)

    def peer(k):
        return {"rows": row + OFFSETS[k][0], "cols": col + OFFSETS[k][1]}

    for k in range(8):
        @pl.when(exists[k])
        def _():
            pl.semaphore_signal(barrier, inc=1, device_id=peer(k), device_id_type=pl.DeviceIdType.MESH)

    lane = lax.broadcasted_iota(jnp.int32, (8, LANES), 1)
    sub = lax.broadcasted_iota(jnp.int32, (8, LANES), 0)
    lane_c = lax.broadcasted_iota(jnp.int32, (crows, LANES), 1)
    middle_lanes = jnp.logical_and(lane_c >= LANES // 4, lane_c < 3 * LANES // 4)

    SIDES, UPDOWN = (0, 1, 3, 4, 5, 7), (2, 6)

    def halo_rows(k):
        return zp.at[pl.ds(1, blocks), pl.ds(8 + rows if k == 2 else 0, 8), :]

    def edge_rows(k):
        return zp.at[pl.ds(1, blocks), pl.ds(rows if k == 2 else 8, 8), :]

    for k in range(8):
        @pl.when(jnp.logical_not(exists[k]))
        def _():
            if k in UPDOWN:
                region = halo_rows(k)
                region[...] = jnp.full(region.shape, OUTSIDE, F32)
                vrecv[k // 4, 0:crows, :] = jnp.full((crows, LANES), OUTSIDE, F32)
                vrecv[k // 4, crows:2 * crows, :] = jnp.zeros((crows, LANES), F32)
            else:
                srecv[k, 0:crows, :] = jnp.where(middle_lanes, 0.0, OUTSIDE)
                srecv[k, crows:crows + 8, :] = jnp.full((8, LANES), OUTSIDE, F32)

    ones[...] = (
        lax.broadcasted_iota(jnp.int32, (cols, LANES), 0) // 8 == lax.broadcasted_iota(jnp.int32, (cols, LANES), 1)
    ).astype(F32).astype(jnp.bfloat16)

    for load in loads:
        load[0].wait()

    packed = jnp.zeros((8, LANES), F32)
    for g in range(groups):
        at = pl.ds(8 + 8 * g, 8)
        edges = jnp.where(lane < LANES // 2, zp[1, at, :], zp[blocks, at, :])
        zp[rim, at, :] = edges
        packed = jnp.where(lane // 4 == g, pltpu.roll(edges, (2 + 4 * g) % LANES, 1), packed)
    side[crows:crows + 8, :] = packed

    pl.semaphore_wait(barrier, functools.reduce(jnp.add, [there.astype(jnp.int32) for there in exists]))

    def copies(k, arriving=False):
        slot = k if arriving else (k + 4) % 8

        def remote(src, dst, extra):
            return pltpu.make_async_remote_copy(
                src_ref=src, dst_ref=dst, send_sem=send_sem.at[k + extra], recv_sem=recv_sem.at[slot + extra],
                device_id=peer(k), device_id_type=pl.DeviceIdType.MESH)

        if k in UPDOWN:
            return remote(edge_rows(k), halo_rows(slot), 8), remote(coarse, vrecv.at[slot // 4], 0)
        fine, wide = pl.ds(crows, 8), pl.ds(0, crows)
        return (remote(side.at[fine, :], srecv.at[slot, fine, :], 8),
                remote(side.at[wide, :], srecv.at[slot, wide, :], 0))

    def send(which):
        for k in (1, 3, 5, 7, 0, 4, 2, 6):
            @pl.when(exists[k])
            def _():
                copies(k)[which].start()

    send(0)

    total = jnp.zeros((4 * crows, LANES), F32)
    for j in range(blocks):
        loads[j][1].wait()
        height_sum = jnp.zeros((crows, LANES), F32)
        count_sum = jnp.zeros((crows, LANES), F32)
        for s in range(8):
            valid = mask[j, pl.ds(s, crows, stride=8), :].astype(F32)
            height_sum = height_sum + valid * zp[j + 1, pl.ds(8 + s, crows, stride=8), :]
            count_sum = count_sum + valid
        high = height_sum.astype(jnp.bfloat16)
        rest = height_sum - high.astype(F32)
        middle = rest.astype(jnp.bfloat16)
        low = (rest - middle.astype(F32)).astype(jnp.bfloat16)
        stacked = jnp.concatenate([count_sum.astype(jnp.bfloat16), high, middle, low], axis=0)
        total = total + jnp.dot(stacked, ones[j * LANES:(j + 1) * LANES, :], preferred_element_type=F32)
    counts = total[0:crows]
    heights = total[crows:2 * crows] + (total[2 * crows:3 * crows] + total[3 * crows:])
    overview = heights / (counts + 1.0)
    runoff = counts * (1.0 / 64.0)

    side[0:crows, :] = jnp.where(middle_lanes, pltpu.roll(runoff, LANES // 2, 1), overview)
    coarse[0:crows, :] = overview
    coarse[crows:2 * crows, :] = runoff

    send(1)

    tie_load.wait()
    coef = coefficients(tie_ref)

    def beside_heights(at, around):
        for j, before, after in around:
            line = [zp[b, at, :] for b in (before, j, after)]
            zl[j, at, :] = shift_lanes(*line, -1, lane)
            zr[j, at, :] = shift_lanes(*line, 1, lane)

    by_column = {-1: zl, 0: zp, 1: zr}
    scale_by_column = {-1: rl, 0: recip, 1: rr}

    def first_pass(g, around):
        done = {}
        middle_at = pl.ds(8 * g + 7, 8)
        for j, before, after in around:
            here = zp[j, middle_at, :]
            summed = jnp.full((8, LANES), RETENTION, F32)
            for k, (off_row, off_col) in enumerate(OFFSETS):
                beside = by_column[off_col][j, pl.ds(8 * g + 7 + off_row, 8), :]
                summed = summed + coef[k] * jnp.maximum(here - beside, 0.0)
            done[j] = 1.0 / summed
            recip[j, middle_at, :] = done[j]
        for j, before, after in around:
            line = [done.get(b, done[j]) for b in (before, j, after)]
            rl[j, middle_at, :] = shift_lanes(*line, -1, lane)
            rr[j, middle_at, :] = shift_lanes(*line, 1, lane)

    def second_pass(g, around, store):
        for j, before, after in around:
            here = zp[j, pl.ds(8 * g + 8, 8), :]
            inside, outer = {}, {}
            for step_col in (-1, 0, 1):
                terms = {}
                for step_row in (-1, 0, 1):
                    if (step_row, step_col) == (0, 0):
                        continue
                    k = OFFSETS.index((-step_row, -step_col))
                    at = pl.ds(8 * g + 8 + step_row, 8)
                    source = by_column[step_col][j, at, :]
                    scale = scale_by_column[step_col][j, at, :]
                    terms[step_row] = coef[k] * jnp.maximum(source - here, 0.0) * scale
                inside[step_col] = jnp.where(sub == 0, 0.0, terms[-1]) + jnp.where(sub == 7, 0.0, terms[1])
                if step_col != 0:
                    inside[step_col] = inside[step_col] + terms[0]
                outer[step_col] = jnp.where(sub == 0, terms[-1], jnp.where(sub == 7, terms[1], 0.0))
            first, last = (lane & 7) == 0, (lane & 7) == 7
            for number, field in enumerate((inside, outer)):
                store(g, j, 2 * number, field[0] + jnp.where(first, 0.0, field[-1]) + jnp.where(last, 0.0, field[1]))
                store(g, j, 2 * number + 1, jnp.where(first, field[-1], jnp.where(last, field[1], 0.0)))

    def keep(g, j, number, value):
        parts[number, j - 1, pl.ds(8 * g, 8), :] = value

    def keep_edges(g, j, number, value):
        at = pl.ds(8 * g, 8)
        parts[number, 0, at, :] = jnp.where(lane < 8, value, parts[number, 0, at, :])
        parts[number, blocks - 1, at, :] = jnp.where(lane >= LANES - 8, value, parts[number, blocks - 1, at, :])

    own = [(j, j - 1, j + 1 if j < blocks else ring) for j in range(1, blocks + 1)]
    outside, edges = (ring, blocks, 1), (rim, ring, ring)

    def loop(start, stop, body):
        def step(g, carry):
            body(g)
            return carry

        lax.fori_loop(start, stop, step, 0)

    loop(0, groups, lambda g: beside_heights(pl.ds(pl.multiple_of(8 * g + 8, 8), 8), own))
    loop(1, groups, lambda g: first_pass(g, own))
    loop(1, groups - 1, lambda g: second_pass(g, own, keep))

    def receive(which):
        for k in range(8):
            @pl.when(exists[k])
            def _():
                copies(k, arriving=True)[which].wait_recv()

    receive(0)

    def outside_columns(g, right, left):
        chosen = jnp.where(lane >= 4 * g + 2, srecv[right, crows:crows + 8, :], srecv[left, crows:crows + 8, :])
        return pltpu.roll(chosen, (2 * LANES - 4 * g - 2) % LANES, 1)

    for g in range(groups):
        zp[ring, pl.ds(8 + 8 * g, 8), :] = outside_columns(g, 0, 4)
    zp[ring, 0:8, :] = outside_columns(groups - 1, 7, 5)
    zp[ring, rows + 8:rows + 16, :] = outside_columns(0, 1, 3)
    for at in (0, rows + 8):
        zp[rim, at:at + 8, :] = jnp.where(lane < LANES // 2, zp[1, at:at + 8, :], zp[blocks, at:at + 8, :])
    for at in (0, rows + 8):
        beside_heights(pl.ds(at, 8), own)
    loop(0, groups + 2, lambda g: beside_heights(pl.ds(pl.multiple_of(8 * g, 8), 8), [outside, edges]))
    loop(0, groups + 1, lambda g: first_pass(g, [outside, edges]))
    loop(0, 2, lambda i: first_pass(i * groups, own))
    loop(0, 2, lambda i: second_pass(i * (groups - 1), own, keep))
    loop(0, groups, lambda g: second_pass(g, [edges], keep_edges))

    receive(1)

    half = LANES // 2

    def window(field):
        def beside(right, left):
            a, b = srecv[right, 0:crows, :], srecv[left, 0:crows, :]
            return jnp.where(lane_c < half, a, b) if field == 0 else pltpu.roll(jnp.where(lane_c < half, b, a), half, 1)

        at = slice(field * crows, (field + 1) * crows)
        here = jnp.concatenate([coarse[at, :], beside(0, 4)], axis=1)
        below = jnp.concatenate([vrecv[0, at, :], beside(1, 3)], axis=1)
        above = jnp.concatenate([vrecv[1, at, :], beside(7, 5)], axis=1)
        sub_w = lax.broadcasted_iota(jnp.int32, (8, 2 * LANES), 0)
        mixed = jnp.where(sub_w < 4, below[8:16], above[crows - 16:crows - 8])
        return jnp.concatenate([here, below[0:8], mixed, above[crows - 8:crows]], axis=0)

    z = window(0)
    supply = window(1)
    high = z.shape[0]

    def turn(x, step, axis):
        return x if step == 0 else pltpu.roll(x, (-step) % x.shape[axis], axis)

    turned = {step: turn(z, step, 1) for step in (-1, 0, 1)}
    slopes = []
    for k, (step_row, step_col) in enumerate(OFFSETS):
        slopes.append(coef[k] * jnp.maximum(z - turn(turned[step_col], step_row, 0), 0.0))
    share = 1.0 / (functools.reduce(jnp.add, slopes) + RETENTION)
    weight = {}
    for k, (step_row, step_col) in enumerate(OFFSETS):
        weight[step_row, step_col] = turn(slopes[k] * share, -step_col, 1)
    flow = supply
    for _ in range(ITERS):
        moved = {step: turn(flow, -step, 1) for step in (-1, 0, 1)}
        sums = {}
        for step_row in (-1, 0, 1):
            sums[step_row] = functools.reduce(
                jnp.add, [weight[step_row, c] * moved[c] for c in (-1, 0, 1) if (step_row, c) in weight])
        flow = supply + sums[0] + turn(sums[1], -1, 0) + turn(sums[-1], 1, 0)

    left = turn(flow, -1, 1)[:, :LANES]
    right = turn(flow, 1, 1)[:, :LANES]
    centre = flow[:, :LANES]
    first, last = (lane & 7) == 0, (lane & 7) == 7
    per_block = LANES // 8
    for j in range(blocks):
        index = lane // 8 + j * per_block
        spread = []
        for at in list(range(0, crows, 8)) + [crows, high - 8]:
            mid = take_lanes(centre[at:at + 8], index)
            beside = jnp.where(first, take_lanes(left[at:at + 8], index), take_lanes(right[at:at + 8], index))
            spread.append((mid, beside))
        for g in range(groups):
            def level(number, group):
                where_at = {-1: (len(spread) - 1, 7), groups: (len(spread) - 2, 0)}.get(group, (group // 8, group % 8))
                line = spread[where_at[0]][number][where_at[1]:where_at[1] + 1, :]
                return jnp.broadcast_to(line, (8, LANES))

            at = slice(8 * g, 8 * g + 8)
            value = mask[j, at, :].astype(F32)
            for number in range(2):
                value = value + parts[number, j, at, :] * level(number, g)
                across = jnp.where(sub == 0, level(number, g - 1), level(number, g + 1))
                value = value + parts[2 + number, j, at, :] * across
            out_ref[at, j * LANES:(j + 1) * LANES] = value

    for k in range(8):
        @pl.when(exists[k])
        def _():
            for copy in copies(k):
                copy.wait_send()


def solution(mesh):
    row_devices, col_devices = mesh.shape["rows"], mesh.shape["cols"]

    def on_device(elevation, data_mask, tie_order):
        rows, cols = elevation.shape
        groups, blocks = rows // 8, cols // LANES
        return pl.pallas_call(
            functools.partial(kernel, row_devices, col_devices),
            out_shape=pltpu.VMEM((rows, cols), F32),
            in_specs=[pl.BlockSpec(memory_space=pl.ANY)] * 3,
            out_specs=pl.BlockSpec(memory_space=pltpu.VMEM),
            scratch_shapes=[
                pltpu.SMEM((8,), jnp.int32),
                pltpu.VMEM((blocks + 2, rows + 16, LANES), F32),
                pltpu.VMEM((blocks + 2, rows + 16, LANES), F32),
                pltpu.VMEM((blocks + 2, rows + 16, LANES), F32),
                pltpu.VMEM((blocks, rows, LANES), jnp.int32),
                pltpu.VMEM((blocks + 2, rows + 16, LANES), F32),
                pltpu.VMEM((blocks + 2, rows + 16, LANES), F32),
                pltpu.VMEM((blocks + 2, rows + 16, LANES), F32),
                pltpu.VMEM((4, blocks, rows, LANES), F32),
                pltpu.VMEM((cols, LANES), jnp.bfloat16),
                pltpu.VMEM((2 * groups, LANES), F32),
                pltpu.VMEM((groups + 8, LANES), F32),
                pltpu.VMEM((8, groups + 8, LANES), F32),
                pltpu.VMEM((2, 2 * groups, LANES), F32),
                pltpu.SemaphoreType.DMA((2 * blocks,)),
                pltpu.SemaphoreType.DMA,
                pltpu.SemaphoreType.DMA((16,)),
                pltpu.SemaphoreType.DMA((16,)),
            ],
            compiler_params=pltpu.CompilerParams(collective_id=0, has_side_effects=True, vmem_limit_bytes=61000000),
        )(tie_order, elevation, data_mask)

    return jax.shard_map(
        on_device, mesh=mesh, in_specs=(P("rows", "cols"), P("rows", "cols"), P()),
        out_specs=P("rows", "cols"), check_vma=False)
```
